512 devices in a mesh: dp: 8 (over z_hi, x), seq: 64 (over z_lo, y, core).
Axes of the slice: x: 4, y: 8, z: 8 (z_hi: 2, z_lo: 4; z = z_hi * 4 + z_lo), core: 2. Of those that a mesh axis runs over, the one named last changes fastest.
Arguments:
- queries: bfloat16 [8, 2048, 12288], P('dp', None, 'seq'), may hold values from -360 to 360
- latent: bfloat16 [8, 2048, 576], P('dp', 'seq'), may hold values from -6 to 6
- latent_gain: float32 [512], replicated, may hold values from 0.1 to 1.9
- segments: int32 [8, 2048], P('dp', 'seq'), may hold values from 0 to 7, never falling along the last dimension, each value on 1 to 512 neighbouring positions
- up_weight: bfloat16 [512, 16384], P('dp', 'seq'), may hold values from -0.25 to 0.25
- out_grad: bfloat16 [8, 2048, 8192], P('dp', None, 'seq'), may hold values from -6 to 6
- hess_old: float32 [512, 16384], P('dp', 'seq'), may hold values from 0.01 to 0.3
Outputs:
- attn_out: bfloat16 [8, 2048, 8192], P('dp', None, 'seq')
- hess_new: float32 [512, 16384], P('dp', 'seq')
The draws below stay inside these ranges and needn't reach their ends.
All inputs are finite; a program needn't handle non-finite values.
Results may differ from the reference program's by a relative error of at most 0.0075.
Values may be sent and summed in bfloat16 or wider, within the bound.
No kernel may reach another device: no remote copies, remote signals or barrier semaphores. Data moves between devices by JAX's collectives and lax.ppermute only.
A program may use at most 64 MiB of HBM per device.

```python
import math
import jax
import jax.numpy as jnp
import numpy as np
from jax import lax

D_LAT = 512
D_ROPE = 64
D_NOPE = 128
D_VAL = 128
DOCS = 8
HEADS = 64
SEQ_LEN = 2048
BATCH = 8
DOC_MOST = 512


def latent_values(key):
    latent_key = jax.random.fold_in(key, 7)
    full_shape = (BATCH, SEQ_LEN, D_LAT + D_ROPE)
    values = jnp.clip(jax.random.normal(latent_key, full_shape, jnp.float32), -6.0, 6.0)
    return values.astype(jnp.bfloat16).astype(jnp.float32)


def draw_latent(key, part):
    return latent_values(key).astype(jnp.bfloat16)


def draw_queries(key, part):
    query_width = D_NOPE + D_ROPE
    full_shape = (BATCH, SEQ_LEN, HEADS, query_width)
    base_key = jax.random.fold_in(jax.random.fold_in(key, 11), 0)
    values = jnp.clip(jax.random.normal(base_key, full_shape, jnp.float32), -6.0, 6.0)
    return values.reshape(BATCH, SEQ_LEN, HEADS * query_width).astype(jnp.bfloat16)


def shard_levels(key, shape, cuts, smallest, high):
    loudness = 1.0
    for position, blocks in cuts:
        heights = jax.random.uniform(jax.random.fold_in(jax.random.fold_in(key, 6), position), (blocks,), jnp.float32, smallest / len(cuts), high / len(cuts))
        loudness = loudness * jnp.repeat(jnp.exp(heights), shape[position] // blocks).reshape((-1,) + (1,) * (len(shape) - 1 - position))
    return loudness


def length_profile(count, total, limit, lean):
    loads = [(1 << 20) // math.isqrt(rank ** lean) + 1 for rank in range(2, count + 1)]
    rest, holding = total - limit - (count - 1), [1] * (count - 1)
    while rest > 0:
        movable = [i for i in range(count - 1) if holding[i] < limit]
        whole, remaining = sum([loads[i] for i in movable]), rest
        for i in movable:
            addition = min(limit - holding[i], max(1, remaining * loads[i] // whole), rest)
            holding[i] = holding[i] + addition
            rest = rest - addition
    return np.array([limit] + holding)


def ragged(stream_key, count, total, limit, lean):
    if count == 2:
        one = jax.random.randint(stream_key, (), max(1, total - limit), min(limit, total - 1) + 1)
        return jnp.stack([one, total - one])
    lengths = jnp.asarray(length_profile(count, total, limit, lean), jnp.int32)
    twos = (count - 1) // 2
    giver, sink = lengths[1:1 + 2 * twos:2], lengths[2:2 + 2 * twos:2]
    margin = jnp.minimum(giver - 1, limit - sink)
    moved = jax.random.randint(jax.random.fold_in(stream_key, 1), (twos,), 0, 1 << 20) % (margin + 1)
    lengths = lengths.at[1:1 + 2 * twos:2].set(giver - moved).at[2:2 + 2 * twos:2].set(sink + moved)
    return lengths[jax.random.permutation(jax.random.fold_in(stream_key, 2), count)]


def bell_draw(stream_key, extent, scale, bound, pieces=(), kind=jnp.bfloat16):
    array = scale * jax.random.normal(stream_key, extent, jnp.float32)
    if pieces:
        array = array * shard_levels(stream_key, extent, pieces, -0.22, 0.18)
    return jnp.clip(array, -bound, bound).astype(kind)


def setup_inputs(seed: int = 0) -> dict:
    splits = jax.random.split(jax.random.key(seed), 8)
    return {
        "queries": draw_queries(jax.random.fold_in(splits[7], 71), 0),
        "latent": draw_latent(jax.random.fold_in(splits[7], 71), 0),
        "latent_gain": jnp.clip(1.0 + 0.18 * jax.random.normal(splits[2], (D_LAT,), jnp.float32), 0.1, 1.9),
        "segments": jax.vmap(lambda own: jnp.searchsorted(jnp.cumsum(ragged(own, DOCS, SEQ_LEN, DOC_MOST, 1)), jnp.arange(SEQ_LEN), side="right"))(jax.random.split(splits[3], BATCH)).reshape((BATCH, SEQ_LEN)).astype(jnp.int32),
        "up_weight": bell_draw(splits[4], (D_LAT, HEADS * (D_NOPE + D_VAL)), D_LAT ** -0.5, 0.25, ((0, 8), (1, 64))),
        "out_grad": bell_draw(splits[5], (BATCH, SEQ_LEN, HEADS * D_VAL), 1.0, 6.0, ((0, 8), (2, 64))),
        "hess_old": jnp.clip(jnp.exp(math.log(0.3) - 3.4011974 * jax.random.uniform(splits[6], (D_LAT, HEADS * (D_NOPE + D_VAL)), jnp.float32) ** shard_levels(splits[6], (D_LAT, HEADS * (D_NOPE + D_VAL)), ((0, 8), (1, 64)), -0.2, 0.2)), 0.01, 0.3),
    }


epsilon = 1e-06
ema_decay = 0.99
rope_base = 10000.0
masked_score = -1e+30

def doc_positions(seg_ids):
    length = seg_ids.shape[0]
    places = jnp.arange(length, dtype=jnp.int32)
    starts_here = jnp.concatenate([jnp.ones((1,), dtype=bool), seg_ids[1:] != seg_ids[:-1]])
    starts = lax.cummax(jnp.where(starts_here, places, jnp.zeros_like(places)), axis=0)
    return places - starts

def rotate_pairs(values_in, positions):
    half_width = values_in.shape[-1] // 2
    steps_up = jnp.arange(half_width, dtype=jnp.float32)
    frequency = rope_base ** (-(2.0 * steps_up) / values_in.shape[-1])
    angles = positions.astype(jnp.float32)[:, None] * frequency[None, :]
    cosine = jnp.cos(angles)
    sine_term = jnp.sin(angles)
    first_half = values_in[:, :half_width]
    second = values_in[:, half_width:]
    return jnp.concatenate([first_half * cosine - second * sine_term, second * cosine + first_half * sine_term], axis=1)

def normalize(latent_rows, latent_gain):
    compressed = latent_rows[:, :D_LAT].astype(jnp.float32)
    spread = lax.optimization_barrier(jnp.mean(compressed * compressed, axis=-1, keepdims=True))
    return (compressed * lax.rsqrt(spread + epsilon) * latent_gain).astype(jnp.bfloat16)

def attend_head(query_head, out_head, normed, key_rope, weight_head, positions, allowed):
    score_scale = (D_NOPE + D_ROPE) ** (-0.5)
    q_nope = query_head[:, :D_NOPE]
    q_rope = rotate_pairs(query_head[:, D_NOPE:].astype(jnp.float32), positions).astype(jnp.bfloat16)
    q_full = jnp.concatenate([q_nope, q_rope], axis=1)
    key_nope = jnp.dot(normed, weight_head[:, :D_NOPE], preferred_element_type=jnp.float32).astype(jnp.bfloat16)
    value_rows = jnp.dot(normed, weight_head[:, D_NOPE:], preferred_element_type=jnp.float32).astype(jnp.bfloat16)
    key_full = jnp.concatenate([key_nope, key_rope], axis=1)
    scores = jnp.dot(q_full, key_full.T, preferred_element_type=jnp.float32) * score_scale
    scores = jnp.where(allowed, scores, masked_score)
    row_max = lax.optimization_barrier(jnp.max(scores, axis=1, keepdims=True))
    expo_rows = jnp.where(allowed, jnp.exp(scores - row_max), 0.0)
    prob_rows = expo_rows / lax.optimization_barrier(jnp.sum(expo_rows, axis=1, keepdims=True))
    prob_low = prob_rows.astype(jnp.bfloat16)
    output = jnp.dot(prob_low, value_rows, preferred_element_type=jnp.float32)
    delta_rows = lax.optimization_barrier(jnp.sum(out_head.astype(jnp.float32) * output, axis=1, keepdims=True))
    value_grad = jnp.dot(prob_low.T, out_head, preferred_element_type=jnp.float32).astype(jnp.bfloat16)
    prob_grad = jnp.dot(out_head, value_rows.T, preferred_element_type=jnp.float32)
    score_grad = (prob_rows * (prob_grad - delta_rows)).astype(jnp.bfloat16)
    key_grad = (jnp.dot(score_grad.T, q_nope, preferred_element_type=jnp.float32) * score_scale).astype(jnp.bfloat16)
    gradient = jnp.dot(normed.T, jnp.concatenate([key_grad, value_grad], axis=1), preferred_element_type=jnp.float32)
    return (output.astype(jnp.bfloat16), gradient)

def one_sequence(query_seq, latent_seq, seg_ids, grad_seq, up_weight, latent_gain):
    positions = doc_positions(seg_ids)
    normed = normalize(latent_seq, latent_gain)
    key_rope = rotate_pairs(latent_seq[:, D_LAT:].astype(jnp.float32), positions).astype(jnp.bfloat16)
    places = jnp.arange(SEQ_LEN, dtype=jnp.int32)
    allowed = (places[None, :] <= places[:, None]) & (seg_ids[None, :] == seg_ids[:, None])
    query_width = D_NOPE + D_ROPE
    pair_width = D_NOPE + D_VAL

    def per_head(head_index):
        query_head = lax.dynamic_slice_in_dim(query_seq, head_index * query_width, query_width, 1)
        out_head = lax.dynamic_slice_in_dim(grad_seq, head_index * D_VAL, D_VAL, 1)
        weight_head = lax.dynamic_slice_in_dim(up_weight, head_index * pair_width, pair_width, 1)
        return attend_head(query_head, out_head, normed, key_rope, weight_head, positions, allowed)
    outputs, gradients = lax.map(per_head, jnp.arange(HEADS, dtype=jnp.int32))
    attention = jnp.transpose(outputs, (1, 0, 2)).reshape(SEQ_LEN, HEADS * D_VAL)
    grad_all = jnp.transpose(gradients, (1, 0, 2)).reshape(D_LAT, HEADS * pair_width)
    return (attention, grad_all)

def reference(queries, latent, latent_gain, segments, up_weight, out_grad, hess_old):

    def per_seq(carry, index):
        attention, grad_all = one_sequence(queries[index], latent[index], segments[index], out_grad[index], up_weight, latent_gain)
        return (carry + grad_all, attention)
    start_total = jnp.zeros((D_LAT, HEADS * (D_NOPE + D_VAL)), jnp.float32)
    gradient, attn_out = lax.scan(per_seq, start_total, jnp.arange(BATCH, dtype=jnp.int32))
    hess_new = ema_decay * hess_old + (1.0 - ema_decay) * gradient * gradient
    return (attn_out, hess_new)
```

```python
import math

import jax
import jax.numpy as jnp
import numpy as np
from jax import lax
from jax.experimental import pallas as pl
from jax.experimental.pallas import tpu as pltpu
from jax.sharding import Mesh
from jax.sharding import PartitionSpec as P

D_LAT = 512
D_ROPE = 64
D_NOPE = 128
D_VAL = 128
D_ROW = 640
BLOCK = 256
SEQ = ("zl", "y", "c")
DP = ("zh", "x")

epsilon = 1e-06
ema_decay = 0.99
rope_base = 10000.0
masked_score = -1e30
score_scale = (D_NOPE + D_ROPE) ** (-0.5)
f32 = jnp.float32
bf16 = jnp.bfloat16


def shifted(x, axis, step):
    size = lax.axis_size(axis)
    return lax.ppermute(x, axis, [(i, (i + step) % size) for i in range(size)])


def copy_for_each(x, axis):
    size = lax.axis_size(axis)
    return lax.all_to_all(jnp.broadcast_to(x[None], (size, *x.shape)), axis, 0, 0, tiled=True)


def normalize(latent_rows, latent_gain):
    compressed = latent_rows[:, :D_LAT].astype(f32)
    spread = jnp.mean(compressed * compressed, axis=-1, keepdims=True)
    return (compressed * lax.rsqrt(spread + epsilon) * latent_gain).astype(bf16)


def nt(a, b):
    return lax.dot_general(a, b, (((1,), (1,)), ((), ())), preferred_element_type=f32)


def nn(a, b):
    return lax.dot_general(a, b, (((1,), (0,)), ((), ())), preferred_element_type=f32)


def tn(a, b):
    return lax.dot_general(a, b, (((0,), (0,)), ((), ())), preferred_element_type=f32)


Y_OFFSETS = (-3, 0, 3, -4, -1, 2, -2, 1)


def constants():
    half = D_ROPE // 2
    freq = rope_base ** (-(2.0 * np.arange(half)) / D_ROPE)
    freq_row = np.zeros((1, 128), np.float32)
    freq_row[0, :half] = freq
    freq_row[0, half:D_ROPE] = freq
    angles = np.arange(BLOCK)[:, None] * np.concatenate([freq, freq])[None, :]
    table = np.zeros((BLOCK, 256), np.float32)
    table[:, :D_ROPE] = np.cos(angles)
    table[:, 128 : 128 + D_ROPE] = np.sin(angles)
    pick = np.zeros((128, 384), np.float32)
    for i in range(half):
        pick[i, i] = 1.0
        pick[half + i, half + i] = 1.0
        pick[half + i, 128 + i] = -1.0
        pick[i, 128 + half + i] = 1.0
    pick[D_ROPE, 256:] = 1.0
    return freq_row, table, pick


def kernel(
    place, mine, other, queries, grads, weight, freq, table, pick,
    out, gradient,
    lat, hot, key, query, val, val_t, starts, key_grad, val_grad, firsts,
):
    length = lat.shape[0]
    blocks = length // BLOCK
    y, c = place[0], place[1]
    own = mine.shape[0] // (4 * 8)
    for z in range(4):
        for j, away in enumerate(Y_OFFSETS):
            at = (z * 8 + lax.rem(y + (away + 8), 8)) * (2 * own)
            rows = slice((j * 4 + z) * own, (j * 4 + z + 1) * own)
            lat[pl.ds(pl.multiple_of(at + c * own, own), own), :] = mine[rows, :]
            lat[pl.ds(pl.multiple_of(at + (1 - c) * own, own), own), :] = other[rows, :]

    lane = lax.broadcasted_iota(jnp.int32, (BLOCK, 128), 1)
    row = lax.broadcasted_iota(jnp.int32, (BLOCK, 128), 0)
    doc = (lane & 7).astype(f32)
    first = jnp.full((1, 128), 8192, jnp.int32)
    for i in range(blocks):
        at = i * BLOCK
        number = nn(lat[at : at + BLOCK, D_LAT:], pick[:, 256:])
        here = number == doc
        hot[at : at + BLOCK, :] = jnp.where(here, 1.0, 0.0).astype(bf16)
        first = jnp.minimum(
            first, jnp.min(jnp.where(here, row + at, 8192), axis=0, keepdims=True)
        )
    lane8 = lax.broadcasted_iota(jnp.int32, (8, 128), 1)
    row8 = lax.broadcasted_iota(jnp.int32, (8, 128), 0)
    first8 = jnp.broadcast_to(first, (8, 128))
    column = jnp.sum(jnp.where(lane8 == row8, first8, 0).astype(f32), axis=1, keepdims=True)
    low = first8 & 255
    split = jnp.where(lane8 < 8, first8 - low, jnp.where(lane8 < 16, low, 0))
    split = split.astype(f32).astype(bf16)

    @pl.loop(0, blocks)
    def prepare(i):
        at = pl.multiple_of(i * BLOCK, BLOCK)
        rows = pl.ds(at, BLOCK)
        marks = hot[rows, :]
        begun = nt(split, marks)
        starts[:, rows] = begun
        firsts[i] = begun[0, 0].astype(jnp.int32)
        theta = (column - lax.convert_element_type(at, f32)) * freq[...]
        both = jnp.concatenate([jnp.cos(theta), jnp.sin(theta)], axis=1)
        high = both.astype(bf16).astype(f32)
        middle = (both - high).astype(bf16).astype(f32)
        last = both - high - middle
        parts = jnp.concatenate([high, middle, last, jnp.zeros_like(both)], axis=0).astype(bf16)
        turn = nn(marks[:, :32], parts)
        cos_s, sin_s = turn[:, :128], turn[:, 128:]
        cos_b, sin_b = table[:, :128], table[:, 128:]
        cosine = cos_b * cos_s + sin_b * sin_s
        sine = sin_b * cos_s - cos_b * sin_s
        raw = nn(lat[rows, D_LAT:], pick[:, :256])
        key[rows, D_NOPE:] = (raw[:, :128] * cosine + raw[:, 128:] * sine).astype(bf16)
        raw = nn(queries[rows, D_NOPE:], pick[:D_ROPE, :256])
        query[rows, :D_NOPE] = queries[rows, :D_NOPE]
        query[rows, D_NOPE:] = (raw[:, :128] * cosine + raw[:, 128:] * sine).astype(bf16)
        pair = nn(lat[rows, :D_LAT], weight[...])
        key[rows, :D_NOPE] = pair[:, :D_NOPE].astype(bf16)
        val[rows, :] = pair[:, D_NOPE:].astype(bf16)
        val_t[:, rows] = pair[:, D_NOPE:].T.astype(bf16)
        key_grad[rows, :] = jnp.zeros((BLOCK, D_NOPE), f32)
        val_grad[rows, :] = jnp.zeros((BLOCK, D_VAL), f32)

    token = lax.broadcasted_iota(jnp.int32, (BLOCK, BLOCK), 0)
    asker = lax.broadcasted_iota(jnp.int32, (BLOCK, BLOCK), 1)

    def attend(i, count):
        at = pl.multiple_of(i * BLOCK, BLOCK)
        rows = pl.ds(at, BLOCK)
        begun = starts[0:1, rows].astype(jnp.int32)
        q_full = query[rows, :]
        grad = grads[rows, :]
        spans = [pl.ds(pl.multiple_of(at - (count - 1 - j) * BLOCK, BLOCK), BLOCK) for j in range(count)]
        scores = []
        for j, span in enumerate(spans):
            s = nt(key[span, :], q_full) * (score_scale * math.log2(math.e))
            allowed = token >= begun - (at - (count - 1 - j) * BLOCK)
            if j == count - 1:
                allowed = allowed & (token <= asker)
            scores.append(jnp.where(allowed, s, masked_score))
        top = jnp.max(scores[0], axis=0, keepdims=True)
        for s in scores[1:]:
            top = jnp.maximum(top, jnp.max(s, axis=0, keepdims=True))
        expo = [jnp.exp2(s - top) for s in scores]
        total = jnp.sum(expo[0], axis=0, keepdims=True)
        for e in expo[1:]:
            total = total + jnp.sum(e, axis=0, keepdims=True)
        inverse = 1.0 / total
        probs = [e * inverse for e in expo]
        lows = [p.astype(bf16) for p in probs]
        prob_grads = [nt(val[span, :], grad) for span in spans]
        delta = jnp.zeros((1, BLOCK), f32)
        for p, g in zip(lows, prob_grads):
            delta = delta + jnp.sum(p.astype(f32) * g, axis=0, keepdims=True)
        result = jnp.zeros((D_VAL, BLOCK), f32)
        for j, span in enumerate(spans):
            result = result + nn(val_t[:, span], lows[j])
            val_grad[span, :] += nn(lows[j], grad)
            score_grad = (probs[j] * (prob_grads[j] - delta)).astype(bf16)
            key_grad[span, :] += nn(score_grad, q_full[:, :D_NOPE])
        out[rows, :] = result.T.astype(bf16)

    @pl.loop(0, blocks)
    def attention(i):
        at = i * BLOCK
        start = firsts[i]
        count = 1 + (start < at).astype(jnp.int32) + (start < at - BLOCK).astype(jnp.int32)
        for n in (1, 2, 3):

            @pl.when(count == n)
            def _():
                attend(i, n)

    total = jnp.zeros((D_LAT, 256), f32)
    for i in range(blocks):
        rows = slice(i * BLOCK, (i + 1) * BLOCK)
        columns = jnp.concatenate([key_grad[rows, :] * score_scale, val_grad[rows, :]], axis=1)
        total = total + tn(lat[rows, :D_LAT], columns.astype(bf16))
    gradient[...] = total.astype(bf16)


def head(place, mine, other, queries, grads, weight):
    length = queries.shape[0]
    freq, table, pick = constants()
    vmem = pl.BlockSpec(memory_space=pltpu.VMEM)
    return pl.pallas_call(
        kernel,
        out_shape=(
            jax.ShapeDtypeStruct((length, D_VAL), bf16),
            jax.ShapeDtypeStruct((D_LAT, D_NOPE + D_VAL), bf16),
        ),
        in_specs=[pl.BlockSpec(memory_space=pltpu.SMEM)] + [vmem] * 8,
        out_specs=(vmem, vmem),
        scratch_shapes=[
            pltpu.VMEM((length, D_ROW), bf16),
            pltpu.VMEM((length, 128), bf16),
            pltpu.VMEM((length, 256), bf16),
            pltpu.VMEM((length, 256), bf16),
            pltpu.VMEM((length, D_VAL), bf16),
            pltpu.VMEM((D_VAL, length), bf16),
            pltpu.VMEM((8, length), f32),
            pltpu.VMEM((length, D_NOPE), f32),
            pltpu.VMEM((length, D_VAL), f32),
            pltpu.SMEM((length // BLOCK,), jnp.int32),
        ],
        compiler_params=pltpu.CompilerParams(vmem_limit_bytes=48 * 1024 * 1024),
        name="head",
    )(place, mine, other, queries, grads, weight, jnp.asarray(freq), jnp.asarray(table), jnp.asarray(pick, bf16))


def local(queries, latent, latent_gain, segments, up_weight, out_grad, hess_old):
    rows = latent.shape[1]
    normed = normalize(latent[0], latent_gain)
    number = jnp.broadcast_to(segments[0][:, None], (rows, D_ROW - D_LAT - D_ROPE)).astype(bf16)
    mine = jnp.concatenate([normed, latent[0][:, D_LAT:], number], axis=1)

    weight = jnp.stack([up_weight, shifted(up_weight, "zh", 1)])
    line = copy_for_each(mine, "zl").reshape(-1, D_ROW)
    upper = shifted(line, "y", 3)
    lower = shifted(line, "y", -3)
    three = jnp.concatenate([upper, line, lower], axis=0)
    left = shifted(three, "y", 1)
    right = shifted(three[: 2 * line.shape[0]], "y", -1)
    half = jnp.concatenate([three, left, right], axis=0)
    other = shifted(half, "c", 1)
    weight = copy_for_each(weight, "x")
    up = lax.axis_index("zh")
    weight = jnp.where(up == 0, weight, weight[:, ::-1])
    weight = jnp.swapaxes(weight, 0, 1).reshape(D_LAT, D_NOPE + D_VAL)

    place = jnp.stack([lax.axis_index("y"), lax.axis_index("c")]).astype(jnp.int32)
    attn_out, grad = head(place, half, other, queries[0], out_grad[0], weight)

    share = hess_old.shape[0]
    grad = jnp.swapaxes(grad.reshape(2, 4, share, -1), 0, 1)
    parts = lax.all_to_all(grad, "x", 0, 0, tiled=True)
    summed = jnp.sum(parts.astype(f32), axis=0)
    sent = shifted(jnp.where(up == 0, summed[1], summed[0]).astype(bf16), "zh", 1)
    total = jnp.where(up == 0, summed[0], summed[1]) + sent.astype(f32)
    hess_new = ema_decay * hess_old + (1.0 - ema_decay) * total * total
    return (attn_out[None], hess_new)


def solution(mesh):
    finer = Mesh(mesh.devices.reshape(2, 4, 4, 8, 2), ("zh", "x", "zl", "y", "c"))
    placed = (
        P(DP, None, SEQ),
        P(DP, SEQ, None),
        P(),
        P(DP, SEQ),
        P(DP, SEQ),
        P(DP, None, SEQ),
        P(DP, SEQ),
    )
    return jax.shard_map(
        local,
        mesh=finer,
        in_specs=placed,
        out_specs=(P(DP, None, SEQ), P(DP, SEQ)),
        check_vma=False,
    )
```

```python
import math

import jax
import jax.numpy as jnp
import numpy as np
from jax import lax
from jax.experimental import pallas as pl
from jax.experimental.pallas import tpu as pltpu
from jax.sharding import Mesh
from jax.sharding import PartitionSpec as P

D_LAT = 512
D_ROPE = 64
D_NOPE = 128
D_VAL = 128
D_ROW = 640
BLOCK = 256
SEQ = ("zl", "y", "c")
DP = ("zh", "x")

epsilon = 1e-06
ema_decay = 0.99
rope_base = 10000.0
masked_score = -1e30
score_scale = (D_NOPE + D_ROPE) ** (-0.5)
f32 = jnp.float32
bf16 = jnp.bfloat16


def shifted(x, axis, step):
    size = lax.axis_size(axis)
    return lax.ppermute(x, axis, [(i, (i + step) % size) for i in range(size)])


def copy_for_each(x, axis):
    size = lax.axis_size(axis)
    return lax.all_to_all(jnp.broadcast_to(x[None], (size, *x.shape)), axis, 0, 0, tiled=True)


def row_kernel(latent_in, gain_in, numbers_in, out, latent, gain, numbers, arrived):
    rows = latent.shape[0]
    copies = [
        pltpu.make_async_copy(source, target, arrived.at[i])
        for i, (source, target) in enumerate(
            ((latent_in, latent), (gain_in, gain), (numbers_in, numbers))
        )
    ]
    for copy in copies:
        copy.start()
    for copy in copies:
        copy.wait()
    compressed = latent[:, :D_LAT].astype(f32)
    spread = jnp.mean(compressed * compressed, axis=-1, keepdims=True)
    normed = (compressed * lax.rsqrt(spread + epsilon) * gain[...]).astype(bf16)
    at = lax.broadcasted_iota(jnp.int32, (rows, rows), 0)
    across = lax.broadcasted_iota(jnp.int32, (rows, rows), 1)
    spread_out = jnp.broadcast_to(numbers[...], (rows, rows))
    number = jnp.sum(jnp.where(at == across, spread_out, 0).astype(f32), axis=1, keepdims=True)
    tail = jnp.broadcast_to(number, (rows, D_ROW - D_LAT - D_ROPE)).astype(bf16)
    rope = jnp.concatenate([latent[:, D_LAT:], tail], axis=1)
    for i in range(out.shape[0]):
        out[i, :, :D_LAT] = normed
        out[i, :, D_LAT:] = rope


def rows_to_send(latent, latent_gain, segments, copies):
    return pl.pallas_call(
        row_kernel,
        out_shape=jax.ShapeDtypeStruct((copies, latent.shape[0], D_ROW), bf16),
        in_specs=[pl.BlockSpec(memory_space=pltpu.HBM)] * 3,
        out_specs=pl.BlockSpec(memory_space=pltpu.VMEM),
        scratch_shapes=[
            pltpu.VMEM(latent.shape, bf16),
            pltpu.VMEM((1, D_LAT), f32),
            pltpu.VMEM(segments.shape, jnp.int32),
            pltpu.SemaphoreType.DMA((3,)),
        ],
        compiler_params=pltpu.CompilerParams(vmem_limit_bytes=4 * 1024 * 1024),
        name="rows",
    )(latent, latent_gain[None], segments)


def nt(a, b):
    return lax.dot_general(a, b, (((1,), (1,)), ((), ())), preferred_element_type=f32)


def nn(a, b):
    return lax.dot_general(a, b, (((1,), (0,)), ((), ())), preferred_element_type=f32)


def tn(a, b):
    return lax.dot_general(a, b, (((0,), (0,)), ((), ())), preferred_element_type=f32)


NEAR = tuple((away, z) for away in (-3, 0, 3) for z in range(4))
FAR = (
    (-4, 2), (-4, 3),
    *((away, z) for away in (-1, 2, -2, 1) for z in range(4)),
    (-4, 0), (-4, 1),
)


def constants():
    half = D_ROPE // 2
    freq = rope_base ** (-(2.0 * np.arange(half)) / D_ROPE)
    twice = np.concatenate([freq, freq])
    angles = np.arange(BLOCK)[:, None] * twice[None, :]
    table = np.zeros((BLOCK + 8, 256), np.float32)
    table[:BLOCK, :D_ROPE] = np.cos(angles)
    table[:BLOCK, 128 : 128 + D_ROPE] = np.sin(angles)
    table[BLOCK:, :D_ROPE] = twice
    return table


def picker(size):
    row = lax.broadcasted_iota(jnp.int32, (size, 256), 0)
    lane = lax.broadcasted_iota(jnp.int32, (size, 256), 1)
    half = D_ROPE // 2
    same = (lane == row) & (row < D_ROPE)
    plus = (lane == row + 128 + half) & (row < half)
    minus = (lane == row + 128 - half) & (row >= half) & (row < D_ROPE)
    return jnp.where(same | plus, 1.0, jnp.where(minus, -1.0, 0.0)).astype(bf16)


def stage_kernel(queries_in, grads_in, table_in, parts, grads, table, queries, arrived):
    copies = [
        pltpu.make_async_copy(source, target, arrived.at[i])
        for i, (source, target) in enumerate(
            ((queries_in, queries), (grads_in, grads), (table_in, table))
        )
    ]
    for copy in copies:
        copy.start()
    pick = picker(D_ROPE)
    copies[0].wait()
    for i in range(parts.shape[0] // BLOCK):
        rows = slice(i * BLOCK, (i + 1) * BLOCK)
        parts[rows, :D_NOPE] = queries[:D_NOPE, rows].T
        parts[rows, D_NOPE:] = tn(queries[D_NOPE:, rows], pick).astype(bf16)
    copies[1].wait()
    copies[2].wait()


def staged(queries, grads):
    table = jnp.asarray(constants())
    length = grads.shape[0]
    return pl.pallas_call(
        stage_kernel,
        out_shape=(
            jax.ShapeDtypeStruct((length, D_NOPE + 256), bf16),
            jax.ShapeDtypeStruct(grads.shape, bf16),
            jax.ShapeDtypeStruct(table.shape, f32),
        ),
        in_specs=[pl.BlockSpec(memory_space=pltpu.HBM)] * 3,
        out_specs=(pl.BlockSpec(memory_space=pltpu.VMEM),) * 3,
        scratch_shapes=[pltpu.VMEM(queries.shape, bf16), pltpu.SemaphoreType.DMA((3,))],
        compiler_params=pltpu.CompilerParams(vmem_limit_bytes=8 * 1024 * 1024),
        cost_estimate=pl.CostEstimate(flops=400_000_000, bytes_accessed=4_000_000, transcendentals=0),
        name="stage",
    )(queries, grads, table)


def kernel(
    place, near, far, near_other, far_other, query_parts, grads, table, pieces,
    out, gradient,
    result_rows,
    weight, lat, hot, key, query, val, val_t, starts, key_grad, val_grad, firsts, left,
):
    length = lat.shape[0]
    blocks = length // BLOCK
    y, c = place[0], place[1]
    own = near.shape[0] // len(NEAR)

    def put(source, held, core):
        for k, (away, z) in enumerate(held):
            at = ((z * 8 + lax.rem(y + (away + 8), 8)) * 2 + core) * own
            lat[pl.ds(pl.multiple_of(at, own), own), :] = source[k * own : (k + 1) * own, :]

    put(near, NEAR, c)
    put(far, FAR, c)
    put(far_other, FAR, 1 - c)
    put(near_other, NEAR, 1 - c)
    share = pieces.shape[2]
    for x in range(4):
        for k in range(2):
            at = ((place[2] ^ k) * 4 + x) * share
            weight[pl.ds(pl.multiple_of(at, share), share), :] = pieces[x, k]

    lane = lax.broadcasted_iota(jnp.int32, (BLOCK, 128), 1)
    row = lax.broadcasted_iota(jnp.int32, (BLOCK, 128), 0)
    doc = (lane & 7).astype(f32)
    pick = picker(128)
    spread = jnp.where(row[:128] == D_ROPE, 1.0, 0.0).astype(bf16)
    first = jnp.full((1, 128), 8192, jnp.int32)
    for i in range(blocks):
        at = i * BLOCK
        number = nn(lat[at : at + BLOCK, D_LAT:], spread)
        here = number == doc
        hot[at : at + BLOCK, :] = jnp.where(here, 1.0, 0.0).astype(bf16)
        first = jnp.minimum(
            first, jnp.min(jnp.where(here, row + at, 8192), axis=0, keepdims=True)
        )
    lane8 = lax.broadcasted_iota(jnp.int32, (8, 128), 1)
    row8 = lax.broadcasted_iota(jnp.int32, (8, 128), 0)
    first8 = jnp.broadcast_to(first, (8, 128))
    column = jnp.sum(jnp.where(lane8 == row8, first8, 0).astype(f32), axis=1, keepdims=True)
    low = first8 & 255
    split = jnp.where(lane8 < 8, first8 - low, jnp.where(lane8 < 16, low, 0))
    split = split.astype(f32).astype(bf16)


    @pl.loop(0, blocks, unroll=2)
    def prepare(i):
        at = pl.multiple_of(i * BLOCK, BLOCK)
        rows = pl.ds(at, BLOCK)
        marks = hot[rows, :]
        begun = nt(split, marks)
        starts[:, rows] = begun
        firsts[i] = begun[0, 0].astype(jnp.int32)
        theta = (column - lax.convert_element_type(at, f32)) * table[BLOCK:, :128]
        both = jnp.concatenate([jnp.cos(theta), jnp.sin(theta)], axis=1)
        high = both.astype(bf16).astype(f32)
        middle = (both - high).astype(bf16).astype(f32)
        last = both - high - middle
        parts = jnp.concatenate([high, middle, last, jnp.zeros_like(both)], axis=0).astype(bf16)
        turn = nn(marks[:, :32], parts)
        cos_s, sin_s = turn[:, :128], turn[:, 128:]
        cos_b, sin_b = table[:BLOCK, :128], table[:BLOCK, 128:]
        cosine = cos_b * cos_s + sin_b * sin_s
        sine = sin_b * cos_s - cos_b * sin_s
        raw = nn(lat[rows, D_LAT:], pick)
        key[rows, D_NOPE:] = (raw[:, :128] * cosine + raw[:, 128:] * sine).astype(bf16)
        raw = query_parts[rows, D_NOPE:].astype(f32)
        query[rows, :D_NOPE] = query_parts[rows, :D_NOPE]
        query[rows, D_NOPE:] = (raw[:, :128] * cosine + raw[:, 128:] * sine).astype(bf16)
        pair = nn(lat[rows, :D_LAT], weight[...])
        key[rows, :D_NOPE] = pair[:, :D_NOPE].astype(bf16)
        val[rows, :] = pair[:, D_NOPE:].astype(bf16)
        val_t[:, rows] = pair[:, D_NOPE:].T.astype(bf16)
        key_grad[rows, :] = jnp.zeros((BLOCK, D_NOPE), f32)
        val_grad[rows, :] = jnp.zeros((BLOCK, D_VAL), f32)

    token = lax.broadcasted_iota(jnp.int32, (BLOCK, BLOCK), 0)
    asker = lax.broadcasted_iota(jnp.int32, (BLOCK, BLOCK), 1)

    def attend(i, count):
        at = pl.multiple_of(i * BLOCK, BLOCK)
        rows = pl.ds(at, BLOCK)
        begun = starts[0:1, rows].astype(jnp.int32)
        q_full = query[rows, :]
        grad = grads[rows, :]
        spans = [pl.ds(pl.multiple_of(at - (count - 1 - j) * BLOCK, BLOCK), BLOCK) for j in range(count)]
        scores = []
        for j, span in enumerate(spans):
            s = nt(key[span, :], q_full) * (score_scale * math.log2(math.e))
            allowed = token >= begun - (at - (count - 1 - j) * BLOCK)
            if j == count - 1:
                allowed = allowed & (token <= asker)
            scores.append(jnp.where(allowed, s, masked_score))
        top = jnp.max(scores[0], axis=0, keepdims=True)
        for s in scores[1:]:
            top = jnp.maximum(top, jnp.max(s, axis=0, keepdims=True))
        expo = [jnp.exp2(s - top) for s in scores]
        total = jnp.sum(expo[0], axis=0, keepdims=True)
        for e in expo[1:]:
            total = total + jnp.sum(e, axis=0, keepdims=True)
        inverse = 1.0 / total
        probs = [e * inverse for e in expo]
        lows = [p.astype(bf16) for p in probs]
        prob_grads = [nt(val[span, :], grad) for span in spans]
        delta = jnp.zeros((1, BLOCK), f32)
        for p, g in zip(lows, prob_grads):
            delta = delta + jnp.sum(p.astype(f32) * g, axis=0, keepdims=True)
        result = jnp.zeros((D_VAL, BLOCK), f32)
        for j, span in enumerate(spans):
            result = result + nn(val_t[:, span], lows[j])
            val_grad[span, :] += nn(lows[j], grad)
            score_grad = (probs[j] * (prob_grads[j] - delta)).astype(bf16)
            key_grad[span, :] += nn(score_grad, q_full[:, :D_NOPE])
        result_rows[rows, :] = result.T.astype(bf16)
        pltpu.make_async_copy(result_rows.at[rows, :], out.at[rows, :], left.at[i]).start()

    @pl.loop(0, blocks)
    def attention(i):
        at = i * BLOCK
        start = firsts[i]
        count = 1 + (start < at).astype(jnp.int32) + (start < at - BLOCK).astype(jnp.int32)
        for n in (1, 2, 3):

            @pl.when(count == n)
            def _():
                attend(i, n)

    total = jnp.zeros((D_LAT, 256), f32)
    for i in range(blocks):
        rows = slice(i * BLOCK, (i + 1) * BLOCK)
        columns = jnp.concatenate([key_grad[rows, :] * score_scale, val_grad[rows, :]], axis=1)
        total = total + tn(lat[rows, :D_LAT], columns.astype(bf16))
    gradient[...] = total.astype(bf16).reshape(gradient.shape)
    for i in range(blocks):
        rows = pl.ds(i * BLOCK, BLOCK)
        pltpu.make_async_copy(result_rows.at[rows, :], out.at[rows, :], left.at[i]).wait()


def head(place, near, far, near_other, far_other, query_parts, grads, table, pieces):
    length = grads.shape[0]
    vmem = pl.BlockSpec(memory_space=pltpu.VMEM)
    return pl.pallas_call(
        kernel,
        out_shape=(
            jax.ShapeDtypeStruct((length, D_VAL), bf16),
            jax.ShapeDtypeStruct((8, D_LAT // 8, D_NOPE + D_VAL), bf16),
        ),
        in_specs=[pl.BlockSpec(memory_space=pltpu.SMEM)] + [vmem] * 8,
        out_specs=(pl.BlockSpec(memory_space=pltpu.HBM), vmem),
        scratch_shapes=[
            pltpu.VMEM((length, D_VAL), bf16),
            pltpu.VMEM((D_LAT, D_NOPE + D_VAL), bf16),
            pltpu.VMEM((length, D_ROW), bf16),
            pltpu.VMEM((length, 128), bf16),
            pltpu.VMEM((length, 256), bf16),
            pltpu.VMEM((length, 256), bf16),
            pltpu.VMEM((length, D_VAL), bf16),
            pltpu.VMEM((D_VAL, length), bf16),
            pltpu.VMEM((8, length), f32),
            pltpu.VMEM((length, D_NOPE), f32),
            pltpu.VMEM((length, D_VAL), f32),
            pltpu.SMEM((length // BLOCK,), jnp.int32),
            pltpu.SemaphoreType.DMA((length // BLOCK,)),
        ],
        compiler_params=pltpu.CompilerParams(vmem_limit_bytes=18 * 1024 * 1024),
        cost_estimate=pl.CostEstimate(flops=3_000_000_000, bytes_accessed=8_000_000, transcendentals=2_000_000),
        name="head",
    )(place, near, far, near_other, far_other, query_parts, grads, table, pieces)


def local(queries, latent, latent_gain, segments, up_weight, out_grad, hess_old):
    up = lax.axis_index("zh")
    place = jnp.stack([lax.axis_index("y"), lax.axis_index("c"), up]).astype(jnp.int32)
    weight = shifted(up_weight, "zh", 1)
    sent = rows_to_send(latent[0], latent_gain, segments, 4)
    line = lax.all_to_all(sent, "zl", 0, 0, tiled=True).reshape(-1, D_ROW)
    upper = shifted(line, "y", 3)
    lower = shifted(line, "y", -3)
    weight = jnp.stack([up_weight, weight])
    weight = copy_for_each(weight, "x")
    near = jnp.concatenate([upper, line, lower], axis=0)
    near, weight = lax.optimization_barrier((near, weight))
    left = shifted(near[line.shape[0] // 2 :], "y", 1)
    right = shifted(near[: 5 * line.shape[0] // 2], "y", -1)
    near_other = shifted(near, "c", 1)
    far = jnp.concatenate([left, right], axis=0)
    far_other = shifted(far, "c", 1)
    ready = staged(queries[0].T, out_grad[0])
    attn_out, grad = head(place, near, far, near_other, far_other, *ready, weight)
    parts = lax.all_to_all(grad, DP, 0, 0, tiled=True)
    total = sum(parts[i].astype(f32) for i in range(parts.shape[0]))
    hess_new = ema_decay * hess_old + (1.0 - ema_decay) * total * total
    return (attn_out[None], hess_new)


def solution(mesh):
    finer = Mesh(mesh.devices.reshape(2, 4, 4, 8, 2), ("zh", "x", "zl", "y", "c"))
    placed = (
        P(DP, None, SEQ),
        P(DP, SEQ, None),
        P(),
        P(DP, SEQ),
        P(DP, SEQ),
        P(DP, None, SEQ),
        P(DP, SEQ),
    )
    return jax.shard_map(
        local,
        mesh=finer,
        in_specs=placed,
        out_specs=(P(DP, None, SEQ), P(DP, SEQ)),
        check_vma=False,
    )
```

```python
import math

import jax
import jax.numpy as jnp
import numpy as np
from jax import lax
from jax.experimental import pallas as pl
from jax.experimental.pallas import tpu as pltpu
from jax.sharding import Mesh
from jax.sharding import PartitionSpec as P

D_LAT = 512
D_ROPE = 64
D_NOPE = 128
D_VAL = 128
D_ROW = 640
BLOCK = 256
HEAD_VMEM = 50 * 1024 * 1024
SEQ = ("zl", "y", "c")
DP = ("zh", "x")

epsilon = 1e-06
ema_decay = 0.99
rope_base = 10000.0
masked_score = -1e30
score_scale = (D_NOPE + D_ROPE) ** (-0.5)
f32 = jnp.float32
bf16 = jnp.bfloat16


def shifted(x, axis, step):
    size = lax.axis_size(axis)
    return lax.ppermute(x, axis, [(i, (i + step) % size) for i in range(size)])


def copy_for_each(x, axis):
    size = lax.axis_size(axis)
    return lax.all_to_all(jnp.broadcast_to(x[None], (size, *x.shape)), axis, 0, 0, tiled=True)


def row_kernel(latent_in, gain_in, numbers_in, out, latent, gain, numbers, arrived):
    rows = latent.shape[0]
    copies = [
        pltpu.make_async_copy(source, target, arrived.at[i])
        for i, (source, target) in enumerate(
            ((latent_in, latent), (gain_in, gain), (numbers_in, numbers))
        )
    ]
    for copy in copies:
        copy.start()
    for copy in copies:
        copy.wait()
    compressed = latent[:, :D_LAT].astype(f32)
    spread = jnp.mean(compressed * compressed, axis=-1, keepdims=True)
    normed = (compressed * lax.rsqrt(spread + epsilon) * gain[...]).astype(bf16)
    at = lax.broadcasted_iota(jnp.int32, (rows, rows), 0)
    across = lax.broadcasted_iota(jnp.int32, (rows, rows), 1)
    spread_out = jnp.broadcast_to(numbers[...], (rows, rows))
    number = jnp.sum(jnp.where(at == across, spread_out, 0).astype(f32), axis=1, keepdims=True)
    tail = jnp.broadcast_to(number, (rows, D_ROW - D_LAT - D_ROPE)).astype(bf16)
    rope = jnp.concatenate([latent[:, D_LAT:], tail], axis=1)
    for i in range(out.shape[0]):
        out[i, :, :D_LAT] = normed
        out[i, :, D_LAT:] = rope


def rows_to_send(latent, latent_gain, segments, copies):
    return pl.pallas_call(
        row_kernel,
        out_shape=jax.ShapeDtypeStruct((copies, latent.shape[0], D_ROW), bf16),
        in_specs=[pl.BlockSpec(memory_space=pltpu.HBM)] * 3,
        out_specs=pl.BlockSpec(memory_space=pltpu.VMEM),
        scratch_shapes=[
            pltpu.VMEM(latent.shape, bf16),
            pltpu.VMEM((1, D_LAT), f32),
            pltpu.VMEM(segments.shape, jnp.int32),
            pltpu.SemaphoreType.DMA((3,)),
        ],
        compiler_params=pltpu.CompilerParams(vmem_limit_bytes=60 * 1024 * 1024),
        name="rows",
    )(latent, latent_gain[None], segments)


def nt(a, b):
    return lax.dot_general(a, b, (((1,), (1,)), ((), ())), preferred_element_type=f32)


def nn(a, b):
    return lax.dot_general(a, b, (((1,), (0,)), ((), ())), preferred_element_type=f32)


def tn(a, b):
    return lax.dot_general(a, b, (((0,), (0,)), ((), ())), preferred_element_type=f32)


NEAR = tuple((away, z) for away in (-3, 0, 3) for z in range(4))
FAR = (
    (-4, 2), (-4, 3),
    *((away, z) for away in (-1, 2, -2, 1) for z in range(4)),
    (-4, 0), (-4, 1),
)


def constants():
    half = D_ROPE // 2
    freq = rope_base ** (-(2.0 * np.arange(half)) / D_ROPE)
    twice = np.concatenate([freq, freq])
    angles = np.arange(BLOCK)[:, None] * twice[None, :]
    table = np.zeros((BLOCK + 8, 256), np.float32)
    table[:BLOCK, :D_ROPE] = np.cos(angles)
    table[:BLOCK, 128 : 128 + D_ROPE] = np.sin(angles)
    table[BLOCK:, :D_ROPE] = twice
    return table


def picker(size):
    row = lax.broadcasted_iota(jnp.int32, (size, 256), 0)
    lane = lax.broadcasted_iota(jnp.int32, (size, 256), 1)
    half = D_ROPE // 2
    same = (lane == row) & (row < D_ROPE)
    plus = (lane == row + 128 + half) & (row < half)
    minus = (lane == row + 128 - half) & (row >= half) & (row < D_ROPE)
    return jnp.where(same | plus, 1.0, jnp.where(minus, -1.0, 0.0)).astype(bf16)


def stage_kernel(queries_in, grads_in, table_in, parts, grads, table, queries, arrived):
    copies = [
        pltpu.make_async_copy(source, target, arrived.at[i])
        for i, (source, target) in enumerate(
            ((queries_in, queries), (grads_in, grads), (table_in, table))
        )
    ]
    for copy in copies:
        copy.start()
    pick = picker(D_ROPE)
    copies[0].wait()
    for i in range(parts.shape[0] // BLOCK):
        rows = slice(i * BLOCK, (i + 1) * BLOCK)
        parts[rows, :D_NOPE] = queries[:D_NOPE, rows].T
        parts[rows, D_NOPE:] = tn(queries[D_NOPE:, rows], pick).astype(bf16)
    copies[1].wait()
    copies[2].wait()


def staged(queries, grads):
    table = jnp.asarray(constants())
    length = grads.shape[0]
    return pl.pallas_call(
        stage_kernel,
        out_shape=(
            jax.ShapeDtypeStruct((length, D_NOPE + 256), bf16),
            jax.ShapeDtypeStruct(grads.shape, bf16),
            jax.ShapeDtypeStruct(table.shape, f32),
        ),
        in_specs=[pl.BlockSpec(memory_space=pltpu.HBM)] * 3,
        out_specs=(pl.BlockSpec(memory_space=pltpu.VMEM),) * 3,
        scratch_shapes=[pltpu.VMEM(queries.shape, bf16), pltpu.SemaphoreType.DMA((3,))],
        compiler_params=pltpu.CompilerParams(vmem_limit_bytes=8 * 1024 * 1024),
        cost_estimate=pl.CostEstimate(flops=400_000_000, bytes_accessed=4_000_000, transcendentals=0),
        name="stage",
    )(queries, grads, table)


def kernel(
    place, near, far, near_other_in, far_other, query_parts_in, grads_in, table_in, pieces,
    out, gradient,
    near_other, query_parts, grads, table, arrived, result_rows,
    weight, lat, hot, key, query, val, val_t, starts, key_grad, val_grad, firsts, left,
):
    length = lat.shape[0]
    blocks = length // BLOCK
    y, c = place[0], place[1]
    copies = [
        pltpu.make_async_copy(source, target, arrived.at[i])
        for i, (source, target) in enumerate(
            ((near_other_in, near_other), (table_in, table), (query_parts_in, query_parts), (grads_in, grads))
        )
    ]
    for copy in copies:
        copy.start()
    own = near.shape[0] // len(NEAR)

    def put(source, held, core):
        for k, (away, z) in enumerate(held):
            at = ((z * 8 + lax.rem(y + (away + 8), 8)) * 2 + core) * own
            lat[pl.ds(pl.multiple_of(at, own), own), :] = source[k * own : (k + 1) * own, :]

    put(near, NEAR, c)
    put(far, FAR, c)
    put(far_other, FAR, 1 - c)
    copies[0].wait()
    put(near_other, NEAR, 1 - c)
    share = pieces.shape[2]
    for x in range(4):
        for k in range(2):
            at = ((place[2] ^ k) * 4 + x) * share
            weight[pl.ds(pl.multiple_of(at, share), share), :] = pieces[x, k]

    lane = lax.broadcasted_iota(jnp.int32, (BLOCK, 128), 1)
    row = lax.broadcasted_iota(jnp.int32, (BLOCK, 128), 0)
    doc = (lane & 7).astype(f32)
    pick = picker(128)
    spread = jnp.where(row[:128] == D_ROPE, 1.0, 0.0).astype(bf16)
    first = jnp.full((1, 128), 8192, jnp.int32)
    for i in range(blocks):
        at = i * BLOCK
        number = nn(lat[at : at + BLOCK, D_LAT:], spread)
        here = number == doc
        hot[at : at + BLOCK, :] = jnp.where(here, 1.0, 0.0).astype(bf16)
        first = jnp.minimum(
            first, jnp.min(jnp.where(here, row + at, 8192), axis=0, keepdims=True)
        )
    lane8 = lax.broadcasted_iota(jnp.int32, (8, 128), 1)
    row8 = lax.broadcasted_iota(jnp.int32, (8, 128), 0)
    first8 = jnp.broadcast_to(first, (8, 128))
    copies[1].wait()
    column = jnp.sum(jnp.where(lane8 == row8, first8, 0).astype(f32), axis=1, keepdims=True)
    low = first8 & 255
    split = jnp.where(lane8 < 8, first8 - low, jnp.where(lane8 < 16, low, 0))
    split = split.astype(f32).astype(bf16)


    copies[2].wait()

    @pl.loop(0, blocks, unroll=4)
    def prepare(i):
        at = pl.multiple_of(i * BLOCK, BLOCK)
        rows = pl.ds(at, BLOCK)
        marks = hot[rows, :]
        begun = nt(split, marks)
        starts[:, rows] = begun
        firsts[i] = begun[0, 0].astype(jnp.int32)
        theta = (column - lax.convert_element_type(at, f32)) * table[BLOCK:, :128]
        both = jnp.concatenate([jnp.cos(theta), jnp.sin(theta)], axis=1)
        high = both.astype(bf16).astype(f32)
        middle = (both - high).astype(bf16).astype(f32)
        last = both - high - middle
        parts = jnp.concatenate([high, middle, last, jnp.zeros_like(both)], axis=0).astype(bf16)
        turn = nn(marks[:, :32], parts)
        cos_s, sin_s = turn[:, :128], turn[:, 128:]
        cos_b, sin_b = table[:BLOCK, :128], table[:BLOCK, 128:]
        cosine = cos_b * cos_s + sin_b * sin_s
        sine = sin_b * cos_s - cos_b * sin_s
        raw = nn(lat[rows, D_LAT:], pick)
        key[rows, D_NOPE:] = (raw[:, :128] * cosine + raw[:, 128:] * sine).astype(bf16)
        raw = query_parts[rows, D_NOPE:].astype(f32)
        query[rows, :D_NOPE] = query_parts[rows, :D_NOPE]
        query[rows, D_NOPE:] = (raw[:, :128] * cosine + raw[:, 128:] * sine).astype(bf16)
        pair = nn(lat[rows, :D_LAT], weight[...])
        key[rows, :D_NOPE] = pair[:, :D_NOPE].astype(bf16)
        val[rows, :] = pair[:, D_NOPE:].astype(bf16)
        val_t[:, rows] = pair[:, D_NOPE:].T.astype(bf16)
        key_grad[rows, :] = jnp.zeros((BLOCK, D_NOPE), f32)
        val_grad[rows, :] = jnp.zeros((BLOCK, D_VAL), f32)

    copies[3].wait()
    token = lax.broadcasted_iota(jnp.int32, (BLOCK, BLOCK), 0)
    asker = lax.broadcasted_iota(jnp.int32, (BLOCK, BLOCK), 1)

    def attend(i, count):
        at = pl.multiple_of(i * BLOCK, BLOCK)
        rows = pl.ds(at, BLOCK)
        begun = starts[0:1, rows].astype(jnp.int32)
        q_full = query[rows, :]
        grad = grads[rows, :]
        spans = [pl.ds(pl.multiple_of(at - (count - 1 - j) * BLOCK, BLOCK), BLOCK) for j in range(count)]
        scores = []
        for j, span in enumerate(spans):
            s = nt(key[span, :], q_full) * (score_scale * math.log2(math.e))
            allowed = token >= begun - (at - (count - 1 - j) * BLOCK)
            if j == count - 1:
                allowed = allowed & (token <= asker)
            scores.append(jnp.where(allowed, s, masked_score))
        top = jnp.max(scores[0], axis=0, keepdims=True)
        for s in scores[1:]:
            top = jnp.maximum(top, jnp.max(s, axis=0, keepdims=True))
        expo = [jnp.exp2(s - top) for s in scores]
        total = jnp.sum(expo[0], axis=0, keepdims=True)
        for e in expo[1:]:
            total = total + jnp.sum(e, axis=0, keepdims=True)
        inverse = 1.0 / total
        probs = [e * inverse for e in expo]
        lows = [p.astype(bf16) for p in probs]
        prob_grads = [nt(val[span, :], grad) for span in spans]
        delta = jnp.zeros((1, BLOCK), f32)
        for p, g in zip(lows, prob_grads):
            delta = delta + jnp.sum(p.astype(f32) * g, axis=0, keepdims=True)
        result = jnp.zeros((D_VAL, BLOCK), f32)
        for j, span in enumerate(spans):
            result = result + nn(val_t[:, span], lows[j])
            val_grad[span, :] += nn(lows[j], grad)
            score_grad = (probs[j] * (prob_grads[j] - delta)).astype(bf16)
            key_grad[span, :] += nn(score_grad, q_full[:, :D_NOPE])
        result_rows[rows, :] = result.T.astype(bf16)
        pltpu.make_async_copy(result_rows.at[rows, :], out.at[rows, :], left.at[i]).start()

    @pl.loop(0, blocks)
    def attention(i):
        at = i * BLOCK
        start = firsts[i]
        count = 1 + (start < at).astype(jnp.int32) + (start < at - BLOCK).astype(jnp.int32)
        for n in (1, 2, 3):

            @pl.when(count == n)
            def _():
                attend(i, n)

    total = jnp.zeros((D_LAT, 256), f32)
    for i in range(blocks):
        rows = slice(i * BLOCK, (i + 1) * BLOCK)
        columns = jnp.concatenate([key_grad[rows, :] * score_scale, val_grad[rows, :]], axis=1)
        total = total + tn(lat[rows, :D_LAT], columns.astype(bf16))
    gradient[...] = total.astype(bf16).reshape(gradient.shape)
    for i in range(blocks):
        rows = pl.ds(i * BLOCK, BLOCK)
        pltpu.make_async_copy(result_rows.at[rows, :], out.at[rows, :], left.at[i]).wait()


def head(place, near, far, near_other, far_other, query_parts, grads, table, pieces):
    length = grads.shape[0]
    vmem = pl.BlockSpec(memory_space=pltpu.VMEM)
    hbm = pl.BlockSpec(memory_space=pltpu.HBM)
    return pl.pallas_call(
        kernel,
        out_shape=(
            jax.ShapeDtypeStruct((length, D_VAL), bf16),
            jax.ShapeDtypeStruct((8, D_LAT // 8, D_NOPE + D_VAL), bf16),
        ),
        in_specs=[pl.BlockSpec(memory_space=pltpu.SMEM)] + [vmem, vmem, hbm, vmem, hbm, hbm, hbm, vmem],
        out_specs=(pl.BlockSpec(memory_space=pltpu.HBM), vmem),
        scratch_shapes=[
            pltpu.VMEM(near_other.shape, bf16),
            pltpu.VMEM(query_parts.shape, bf16),
            pltpu.VMEM(grads.shape, bf16),
            pltpu.VMEM(table.shape, f32),
            pltpu.SemaphoreType.DMA((4,)),
            pltpu.VMEM((length, D_VAL), bf16),
            pltpu.VMEM((D_LAT, D_NOPE + D_VAL), bf16),
            pltpu.VMEM((length, D_ROW), bf16),
            pltpu.VMEM((length, 128), bf16),
            pltpu.VMEM((length, 256), bf16),
            pltpu.VMEM((length, 256), bf16),
            pltpu.VMEM((length, D_VAL), bf16),
            pltpu.VMEM((D_VAL, length), bf16),
            pltpu.VMEM((8, length), f32),
            pltpu.VMEM((length, D_NOPE), f32),
            pltpu.VMEM((length, D_VAL), f32),
            pltpu.SMEM((length // BLOCK,), jnp.int32),
            pltpu.SemaphoreType.DMA((length // BLOCK,)),
        ],
        compiler_params=pltpu.CompilerParams(vmem_limit_bytes=HEAD_VMEM),
        cost_estimate=pl.CostEstimate(flops=3_000_000_000, bytes_accessed=8_000_000, transcendentals=2_000_000),
        name="head",
    )(place, near, far, near_other, far_other, query_parts, grads, table, pieces)


def local(queries, latent, latent_gain, segments, up_weight, out_grad, hess_old):
    up = lax.axis_index("zh")
    place = jnp.stack([lax.axis_index("y"), lax.axis_index("c"), up]).astype(jnp.int32)
    weight = shifted(up_weight, "zh", 1)
    sent = rows_to_send(latent[0], latent_gain, segments, 4)
    line = lax.all_to_all(sent, "zl", 0, 0, tiled=True).reshape(-1, D_ROW)
    upper = shifted(line, "y", 3)
    lower = shifted(line, "y", -3)
    weight = jnp.stack([up_weight, weight])
    weight = copy_for_each(weight, "x")
    near = jnp.concatenate([upper, line, lower], axis=0)
    near, weight = lax.optimization_barrier((near, weight))
    left = shifted(near[line.shape[0] // 2 :], "y", 1)
    right = shifted(near[: 5 * line.shape[0] // 2], "y", -1)
    near_other = shifted(near, "c", 1)
    far = jnp.concatenate([left, right], axis=0)
    far_other = shifted(far, "c", 1)
    ready = staged(queries[0].T, out_grad[0])
    attn_out, grad = head(place, near, far, near_other, far_other, *ready, weight)
    parts = lax.all_to_all(grad, DP, 0, 0, tiled=True)
    total = sum(parts[i].astype(f32) for i in range(parts.shape[0]))
    hess_new = ema_decay * hess_old + (1.0 - ema_decay) * total * total
    return (attn_out[None], hess_new)


def solution(mesh):
    finer = Mesh(mesh.devices.reshape(2, 4, 4, 8, 2), ("zh", "x", "zl", "y", "c"))
    placed = (
        P(DP, None, SEQ),
        P(DP, SEQ, None),
        P(),
        P(DP, SEQ),
        P(DP, SEQ),
        P(DP, None, SEQ),
        P(DP, SEQ),
    )
    return jax.shard_map(
        local,
        mesh=finer,
        in_specs=placed,
        out_specs=(P(DP, None, SEQ), P(DP, SEQ)),
        check_vma=False,
    )
```
